16 devices in a mesh: dp: 2 (over y, z), tp: 8 (over x, core).
Axes of the slice: x: 4, y: 2, z: 1, core: 2. Of those that a mesh axis runs over, the one named last changes fastest.
The devices are a block of a 4x4x8 slice.
Arguments:
- x: bfloat16 [2048, 8192], P(('dp', 'tp')), parts along dimension 0
- gain_a: bfloat16 [8192], replicated
- wq: bfloat16 [8192, 8192], P(None, 'tp')
- wk: bfloat16 [8192, 8192], P(None, 'tp')
- wv: bfloat16 [8192, 8192], P(None, 'tp')
- wo: bfloat16 [8192, 8192], P('tp')
- gain_m: bfloat16 [8192], replicated
- w_gate: bfloat16 [8192, 24576], P(None, 'tp')
- w_up: bfloat16 [8192, 24576], P(None, 'tp')
- w_down: bfloat16 [24576, 8192], P('tp')
Outputs:
- output: bfloat16 [2048, 8192], P(('dp', 'tp')), parts along dimension 0
There are 2 independent parts. The reference program is written for one: setup_inputs(seed, part) draws one part's arguments, and reference() takes and returns one part's arrays. A program takes and returns all parts, laid end to end along the dimension named above; an argument that names none is the same for every part.
All inputs are finite; a program needn't handle non-finite values.
Results may differ from the reference program's by a relative error of at most 0.017.
Values are sent between devices in bfloat16 or wider.
A program may use at most 768 MiB of HBM per device.

```python
import jax
import jax.numpy as jnp
from jax import lax

ROWS = 1024
D = 8192
HEADS = 64
KV_HEADS = 64
HEAD = 128
FF = 24576
THETA = 10000


def setup_inputs(seed: int = 0, part: int = 0) -> dict:
    kx, kn, kq, kk, kv, ko, km, kg, ku, kd = jax.random.split(jax.random.key(seed), 10)

    def weights(key, rows, columns):
        return jax.random.normal(key, (rows, columns), jnp.float32) * rows**-0.5

    drawn = {
        "x": jax.random.normal(jax.random.fold_in(kx, part), (ROWS, D), jnp.float32),
        "gain_a": 1 + 0.1 * jax.random.normal(kn, (D,), jnp.float32),
        "wq": 2 * weights(kq, D, HEADS * HEAD),
        "wk": 2 * weights(kk, D, KV_HEADS * HEAD),
        "wv": 4 * weights(kv, D, KV_HEADS * HEAD),
        "wo": weights(ko, HEADS * HEAD, D),
        "gain_m": 1 + 0.1 * jax.random.normal(km, (D,), jnp.float32),
        "w_gate": weights(kg, D, FF),
        "w_up": weights(ku, D, FF),
        "w_down": 2 * weights(kd, FF, D),
    }
    return {k: v.astype(jnp.bfloat16) for k, v in drawn.items()}


def normed(x, gain):
    wide = x.astype(jnp.float32)
    scale = lax.rsqrt(jnp.mean(wide * wide, -1, keepdims=True) + 1e-6)
    return (wide * scale * gain.astype(jnp.float32)).astype(jnp.bfloat16)


def turned(t, place, theta):
    half = t.shape[-1] // 2
    angle = place.astype(jnp.float32)[:, None] * theta ** (-jnp.arange(half, dtype=jnp.float32) / half)
    cos, sin = jnp.cos(angle)[:, None], jnp.sin(angle)[:, None]
    a, b = t[..., :half].astype(jnp.float32), t[..., half:].astype(jnp.float32)
    return jnp.concatenate([a * cos - b * sin, b * cos + a * sin], -1).astype(jnp.bfloat16)


def matmul(a, w):
    return jnp.dot(a, w, preferred_element_type=jnp.float32).astype(jnp.bfloat16)


def einsum(form, a, b):
    return jnp.einsum(form, a.astype(jnp.float32), b.astype(jnp.float32))


def attention(q, k, v):
    scores = einsum("tgsd,ugd->gstu", q, k) * q.shape[-1] ** -0.5
    token = jnp.arange(q.shape[0])
    scores = jnp.where(token[:, None] >= token, scores, -jnp.inf)
    weights = jax.nn.softmax(scores, -1).astype(jnp.bfloat16)
    return einsum("gstu,ugd->tgsd", weights, v).astype(jnp.bfloat16)


def reference(x, gain_a, wq, wk, wv, wo, gain_m, w_gate, w_up, w_down):
    a, place = normed(x, gain_a), jnp.arange(ROWS)
    q = turned(matmul(a, wq).reshape(ROWS, HEADS, HEAD), place, THETA).reshape(ROWS, KV_HEADS, -1, HEAD)
    k = turned(matmul(a, wk).reshape(ROWS, KV_HEADS, HEAD), place, THETA)
    v = matmul(a, wv).reshape(ROWS, KV_HEADS, HEAD)
    seen = attention(q, k, v).reshape(ROWS, HEADS * HEAD)
    h = (x.astype(jnp.float32) + jnp.dot(seen, wo, preferred_element_type=jnp.float32)).astype(jnp.bfloat16)
    b = normed(h, gain_m)
    gate = jnp.dot(b, w_gate, preferred_element_type=jnp.float32)
    up = jnp.dot(b, w_up, preferred_element_type=jnp.float32)
    hidden = (jax.nn.silu(gate) * up).astype(jnp.bfloat16)
    return (h.astype(jnp.float32) + jnp.dot(hidden, w_down, preferred_element_type=jnp.float32)).astype(jnp.bfloat16)
```

```python
import functools

import jax
import jax.numpy as jnp
import numpy as np
from jax import lax
from jax.experimental import pallas as pl
from jax.experimental.pallas import tpu as pltpu
from jax.sharding import PartitionSpec as P

HEAD = 128
THETA = 10000
NEG = -1e30
HIDDEN = 2 * NEG
LOG2E = 1.4426950408889634
VMEM = 67_000_000
MESH = pl.DeviceIdType.MESH
PIECE = 512
F32, BF16 = jnp.float32, jnp.bfloat16


def _dot(a, b, ca, cb):
    return lax.dot_general(a, b, (((ca,), (cb,)), ((), ())), preferred_element_type=F32)


def _place(n):
    me = lax.axis_index("tp")
    chips = n // 2
    chip, core = me // 2, me % 2
    at = lambda step: ((chip + step) % chips) * 2 + core
    return me, core, chip * 2 + 1 - core, at(1), at(chips - 1), at(chips // 2)


def _greet(others):
    barrier = pltpu.get_barrier_semaphore()
    for other in others:
        pl.semaphore_signal(barrier, inc=1, device_id={"tp": other}, device_id_type=MESH)
    pl.semaphore_wait(barrier, len(others))


def _gather_kernel(n, count, finish, tile, x_ref, gain_ref, *rest):
    weights, rest = rest[:count], rest[count:]
    extra, rest = rest[: finish.extra], rest[finish.extra :]
    outs, rest = rest[: finish.outs], rest[finish.outs :]
    xg, acc, wbuf, wsem, osem, ssem, rsem = rest
    pieces, rows, width = xg.shape
    own = rows // n
    half = own // 2
    each = weights[0].shape[1]
    me, core, partner, right, left, opposite = _place(n)

    def weight_copies(k):
        return [
            pltpu.make_async_copy(w.at[pl.ds(k * width, width), :], wbuf.at[k % 2, :, pl.ds(j * each, each)], wsem.at[k % 2, j])
            for j, w in enumerate(weights)
        ]

    for k in range(2):
        for c in weight_copies(k):
            c.start()

    def squares(k, total):
        wide = x_ref[:, pl.ds(k * width, width)].astype(F32)
        return total + jnp.sum(wide * wide, -1, keepdims=True)

    total = lax.fori_loop(0, pieces, squares, jnp.zeros((own, 1), F32))
    scale = lax.rsqrt(total * (1 / (pieces * width)) + 1e-6)
    mine = pl.multiple_of(me * own, own)

    def norm(k, _):
        here = pl.ds(k * width, width)
        xg[k, pl.ds(mine, own), :] = (x_ref[:, here].astype(F32) * scale * gain_ref[:, here].astype(F32)).astype(BF16)

    lax.fori_loop(0, pieces, norm, None)
    _greet((partner, right, left))

    def copy(k, m, owner, low, size, to):
        block = xg.at[k, pl.ds(pl.multiple_of(owner * own + low, half), size), :]
        return pltpu.make_async_remote_copy(block, block, ssem.at[k, m], rsem.at[k, m], device_id={"tp": to}, device_id_type=MESH)

    across = lambda other: other + 1 - 2 * core
    opp2, left2, right2 = across(opposite), across(left), across(right)

    sent = (
        (me, 0, own, partner),
        (me, 0, own, right),
        (me, 0, own, left),
        (left, 0, half, right),
        (right, half, half, left),
        (left, 0, own, partner),
        (right, 0, own, partner),
        (opposite, 0, half, partner),
        (opposite, half, half, partner),
    )
    landed = (
        (partner, 0, own, partner),
        (left, 0, own, partner),
        (right, 0, own, partner),
        (opposite, 0, half, partner),
        (opposite, half, half, partner),
        (left2, 0, own, partner),
        (right2, 0, own, partner),
        (opp2, 0, half, partner),
        (opp2, half, half, partner),
    )

    def start(k, *which):
        for m in which:
            copy(k, m, *sent[m]).start()

    def await_(k, *which):
        for m in which:
            copy(k, m, *landed[m]).wait_recv()

    acc[...] = jnp.zeros_like(acc)

    def step(s, _):
        @pl.when(s < pieces)
        def _():
            start(s, 1, 2, 0)

        @pl.when((s >= 1) & (s <= pieces))
        def _():
            await_(s - 1, 1)
            start(s - 1, 3, 5)
            await_(s - 1, 2)
            start(s - 1, 4, 6)

        @pl.when((s >= 2) & (s <= pieces + 1))
        def _():
            await_(s - 2, 3)
            start(s - 2, 7)
            await_(s - 2, 4)
            start(s - 2, 8)

        @pl.when(s >= 3)
        def _():
            k = s - 3
            await_(k, 0, 5, 6, 7, 8)
            for c in weight_copies(k):
                c.wait()

            def columns(t, _):
                here = pl.ds(pl.multiple_of(t * tile, tile), tile)
                acc[:, here] += _dot(xg[k], wbuf[k % 2, :, here], 1, 0)

            lax.fori_loop(0, acc.shape[1] // tile, columns, None)

            @pl.when(k + 2 < pieces)
            def _():
                for c in weight_copies(k + 2):
                    c.start()

    lax.fori_loop(0, pieces + 3, step, None)
    finish(acc, wbuf, extra, outs, osem)

    def drain(k, _):
        for m in range(len(sent)):
            copy(k, m, *sent[m]).wait_send()

    lax.fori_loop(0, pieces, drain, None)


class _Blocks:
    def __init__(self, values, outs, extra):
        self.values, self.outs, self.extra = values, outs, extra

    def __call__(self, acc, wbuf, extra, outs, osem):
        rows = wbuf.shape[1] // 2
        each = outs[0].shape[1]
        copies = []
        for b in range(4):
            low = (b % 2) * rows

            def columns(t, _):
                here = pl.ds(pl.multiple_of(t * 128, 128), 128)
                wbuf[b // 2, low : low + rows, here] = self.values(acc, extra, b * rows, rows, t)

            lax.fori_loop(0, each * len(outs) // 128, columns, None)
            for j, out in enumerate(outs):
                c = pltpu.make_async_copy(
                    wbuf.at[b // 2, pl.ds(low, rows), pl.ds(j * each, each)], out.at[pl.ds(b * rows, rows), :], osem.at[b, j]
                )
                c.start()
                copies.append(c)
        for c in copies:
            c.wait()


def _gather(n, collective_id, x, gain, weights, finish, tile, extra, out_columns):
    own, depth = x.shape
    rows, each, count = own * n, weights[0].shape[1], len(weights)
    pieces = depth // PIECE
    vmem, hbm = pl.BlockSpec(memory_space=pltpu.VMEM), pl.BlockSpec(memory_space=pl.ANY)
    return pl.pallas_call(
        functools.partial(_gather_kernel, n, count, finish, tile),
        out_shape=[jax.ShapeDtypeStruct((rows, out_columns), BF16)] * finish.outs,
        in_specs=[vmem, vmem] + [hbm] * count + [vmem] * finish.extra,
        out_specs=[hbm] * finish.outs,
        scratch_shapes=[
            pltpu.VMEM((pieces, rows, PIECE), BF16),
            pltpu.VMEM((rows, each * count), F32),
            pltpu.VMEM((2, PIECE, each * count), BF16),
            pltpu.SemaphoreType.DMA((2, count)),
            pltpu.SemaphoreType.DMA((4, finish.outs)),
            pltpu.SemaphoreType.DMA((pieces, 9)),
            pltpu.SemaphoreType.DMA((pieces, 9)),
        ],
        compiler_params=pltpu.CompilerParams(collective_id=collective_id, has_side_effects=True, vmem_limit_bytes=VMEM),
        cost_estimate=pl.CostEstimate(
            flops=2 * rows * depth * each * count, bytes_accessed=2 * depth * each * count, transcendentals=rows * each
        ),
    )(x, gain.reshape(1, -1), *weights, *extra)


def _scatter_kernel(n, a_ref, w_ref, x_ref, o_ref, a_v, wbuf, keep, d_out, d_in, a_out, a_in, b_out, b_in, asem, wsem, ssem, rsem):
    pieces, width = d_in.shape[0], wbuf.shape[2]
    own = keep.shape[2]
    half = own // 2
    chips = n // 2
    me, core, partner, right, left, opposite = _place(n)

    def weight_copy(k):
        here = pl.ds(pl.multiple_of(k * width, width), width)
        return pltpu.make_async_copy(w_ref.at[:, here], wbuf.at[k % 3], wsem.at[k % 3])

    fetch = pltpu.make_async_copy(a_ref, a_v, asem)
    fetch.start()
    for k in range(2):
        weight_copy(k).start()
    _greet((partner, right, left))

    def copy(k, m, source, target, to):
        return pltpu.make_async_remote_copy(source, target, ssem.at[k, m], rsem.at[k, m], device_id={"tp": to}, device_id_type=MESH)

    def cores(k):
        return copy(k, 0, d_out.at[k % 2], d_in.at[k], partner)

    def far(k):
        return [
            copy(k, 1, a_out.at[k % 2, pl.ds(0, half)], a_in.at[k, pl.ds(0, half)], right),
            copy(k, 2, a_out.at[k % 2, pl.ds(half, half)], a_in.at[k, pl.ds(half, half)], left),
        ]

    def near(k):
        return [copy(k, 3, b_out.at[k % 2, 0], b_in.at[k, 0], right), copy(k, 4, b_out.at[k % 2, 1], b_in.at[k, 1], left)]

    def term(k, owner, low=0, size=own):
        here = pl.ds(low, size)
        return keep[k % 4, owner, here, :] + d_in[k, owner // 2, here, :].astype(F32)

    fetch.wait()

    def step(s, _):
        @pl.when(s < pieces)
        def _():
            weight_copy(s).wait()

            @pl.when(s + 2 < pieces)
            def _():
                weight_copy(s + 2).start()

            keep[s % 4] = _dot(a_v[...], wbuf[s % 3], 1, 0).reshape(n, own, width)

            @pl.when(s >= 2)
            def _():
                cores(s - 2).wait_send()

            for q in range(chips):
                d_out[s % 2, q] = keep[s % 4, 2 * q + 1 - core].astype(BF16)

        @pl.when((s >= 1) & (s <= pieces))
        def _():
            k = s - 1
            cores(k).wait_recv()

            @pl.when(k >= 2)
            def _():
                for c in far(k - 2):
                    c.wait_send()

            a_out[k % 2] = term(k, opposite).astype(BF16)

        @pl.when(s < pieces)
        def _():
            cores(s).start()

        @pl.when((s >= 2) & (s <= pieces + 1))
        def _():
            k = s - 2
            for c in far(k):
                c.wait_recv()

            @pl.when(k >= 2)
            def _():
                for c in near(k - 2):
                    c.wait_send()

            b_out[k % 2, 0, pl.ds(0, half)] = (term(k, right, 0, half) + a_in[k, pl.ds(0, half)].astype(F32)).astype(BF16)
            b_out[k % 2, 0, pl.ds(half, half)] = term(k, right, half, half).astype(BF16)
            b_out[k % 2, 1, pl.ds(0, half)] = term(k, left, 0, half).astype(BF16)
            b_out[k % 2, 1, pl.ds(half, half)] = (term(k, left, half, half) + a_in[k, pl.ds(half, half)].astype(F32)).astype(BF16)

        @pl.when((s >= 1) & (s <= pieces))
        def _():
            for c in far(s - 1):
                c.start()

        @pl.when(s >= 3)
        def _():
            k = s - 3
            for c in near(k):
                c.wait_recv()
            here = pl.ds(pl.multiple_of(k * width, width), width)
            total = term(k, me) + b_in[k, 0].astype(F32) + b_in[k, 1].astype(F32)
            o_ref[:, here] = (x_ref[:, here].astype(F32) + total).astype(BF16)

        @pl.when((s >= 2) & (s <= pieces + 1))
        def _():
            for c in near(s - 2):
                c.start()

    lax.fori_loop(0, pieces + 3, step, None)
    for k in (pieces - 2, pieces - 1):
        for c in [cores(k), *far(k), *near(k)]:
            c.wait_send()


def _scatter(n, collective_id, a, w, x):
    rows, depth = a.shape
    own, columns = x.shape
    pieces = columns // PIECE
    vmem, hbm = pl.BlockSpec(memory_space=pltpu.VMEM), pl.BlockSpec(memory_space=pl.ANY)
    return pl.pallas_call(
        functools.partial(_scatter_kernel, n),
        out_shape=jax.ShapeDtypeStruct((own, columns), BF16),
        in_specs=[hbm, hbm, vmem],
        out_specs=vmem,
        scratch_shapes=[
            pltpu.VMEM((rows, depth), BF16),
            pltpu.VMEM((3, depth, PIECE), BF16),
            pltpu.VMEM((4, n, own, PIECE), F32),
            pltpu.VMEM((2, n // 2, own, PIECE), BF16),
            pltpu.VMEM((pieces, n // 2, own, PIECE), BF16),
            pltpu.VMEM((2, own, PIECE), BF16),
            pltpu.VMEM((pieces, own, PIECE), BF16),
            pltpu.VMEM((2, 2, own, PIECE), BF16),
            pltpu.VMEM((pieces, 2, own, PIECE), BF16),
            pltpu.SemaphoreType.DMA,
            pltpu.SemaphoreType.DMA((3,)),
            pltpu.SemaphoreType.DMA((pieces, 5)),
            pltpu.SemaphoreType.DMA((pieces, 5)),
        ],
        compiler_params=pltpu.CompilerParams(collective_id=collective_id, has_side_effects=True, vmem_limit_bytes=VMEM),
        cost_estimate=pl.CostEstimate(flops=2 * rows * depth * columns, bytes_accessed=2 * depth * columns, transcendentals=0),
    )(a, w, x)


def _attention_kernel(q_ref, k_ref, v_ref, o_ref, top_s, mix_s, *, bq, bk, scale):
    heads = top_s.shape[0]
    iq = pl.program_id(0)
    e = scale * LOG2E
    top_s[...] = jnp.full(top_s.shape, NEG, F32)
    mix_s[...] = jnp.zeros(mix_s.shape, F32)
    ones = jnp.ones((8, bk), BF16)
    gap = lax.broadcasted_iota(jnp.int32, (bk, bq), 1) - lax.broadcasted_iota(jnp.int32, (bk, bq), 0)
    part = lambda i: slice(i * HEAD, (i + 1) * HEAD)

    def block(j, masked):
        here = pl.ds(pl.multiple_of(j * bk, bk), bk)
        scores = [_dot(k_ref[here, part(i)], q_ref[:, part(i)], 1, 1) for i in range(heads)]
        weights, keeps = [], []
        for i, s in enumerate(scores):
            if masked:
                s = jnp.where(gap >= j * bk - iq * bq, s, HIDDEN)
            old = top_s[i : i + 1, :]
            top = jnp.maximum(old, s.max(axis=0, keepdims=True))
            top_s[i : i + 1, :] = top
            weights.append(jnp.exp2((s - top) * e).astype(BF16))
            keeps.append(jnp.exp2((old - top) * e))
        for i, (p, keep) in enumerate(zip(weights, keeps)):
            values = jnp.concatenate([v_ref[here, part(i)].T, ones], axis=0)
            mix_s[i] = mix_s[i] * keep + _dot(values, p, 1, 0)

    whole = iq * bq // bk
    lax.fori_loop(0, whole, lambda j, _: block(j, False), None)
    lax.fori_loop(whole, whole + bq // bk, lambda j, _: block(j, True), None)
    for i in range(heads):
        total = mix_s[i, HEAD : HEAD + 1, :]
        o_ref[:, part(i)] = (mix_s[i, :HEAD, :] * (1 / total)).T.astype(BF16)


def _attention(q, k, v, bq=512, bk=256):
    rows, columns = q.shape
    heads = columns // HEAD
    some = pl.BlockSpec((bq, columns), lambda i: (i, 0))
    every = pl.BlockSpec((rows, columns), lambda i: (0, 0))
    return pl.pallas_call(
        functools.partial(_attention_kernel, bq=bq, bk=bk, scale=HEAD**-0.5),
        grid=(rows // bq,),
        in_specs=[some, every, every],
        out_specs=some,
        out_shape=jax.ShapeDtypeStruct((rows, columns), BF16),
        scratch_shapes=[pltpu.VMEM((heads, bq), F32), pltpu.VMEM((heads, HEAD + 8, bq), F32)],
        compiler_params=pltpu.CompilerParams(dimension_semantics=("arbitrary",), vmem_limit_bytes=56 * 2**20),
        cost_estimate=pl.CostEstimate(flops=4 * rows * rows * columns, bytes_accessed=8 * rows * columns, transcendentals=heads * rows * rows),
    )(q, k, v)


def _tables(rows):
    half = HEAD // 2
    rate = (np.float32(THETA) ** (-np.arange(half, dtype=np.float32) / np.float32(half))).astype(np.float32)
    angle = np.arange(rows, dtype=np.float32)[:, None] * rate
    cos, sin = np.cos(angle.astype(np.float64)), np.sin(angle.astype(np.float64))
    return np.concatenate([cos, cos], 1).astype(np.float32), np.concatenate([-sin, sin], 1).astype(np.float32)


def _qkv(acc, extra, low, rows, t):
    here = pl.ds(pl.multiple_of(t * HEAD, HEAD), HEAD)
    value = acc[low : low + rows, here].astype(BF16)
    wide = value.astype(F32)
    cos, sin = (r[low : low + rows, :] for r in extra)
    turned = (wide * cos + pltpu.roll(wide, HEAD // 2, 1) * sin).astype(BF16)
    return jnp.where(t < 2 * acc.shape[1] // (3 * HEAD), turned, value)


def _hidden(acc, extra, low, rows, t):
    here = lambda first: pl.ds(pl.multiple_of(first + t * 128, 128), 128)
    gate, up = acc[low : low + rows, here(0)], acc[low : low + rows, here(acc.shape[1] // 2)]
    return (gate * lax.logistic(gate) * up).astype(BF16)


def solution(mesh):
    n = mesh.shape["tp"]

    def step(x, gain_a, wq, wk, wv, wo, gain_m, w_gate, w_up, w_down):
        rows = x.shape[0] * n
        tables = [jnp.asarray(t) for t in _tables(rows)]
        q, k, v = _gather(n, 0, x, gain_a, (wq, wk, wv), _Blocks(_qkv, 3, 2), 1024, tables, wq.shape[1])
        seen = _attention(q, k, v)
        h = _scatter(n, 1, seen, wo, x)
        (hidden,) = _gather(n, 2, h, gain_m, (w_gate, w_up), _Blocks(_hidden, 1, 0), 2048, (), w_gate.shape[1])
        return _scatter(n, 3, hidden, w_down, h)

    tokens, columns, rows_of = P(("dp", "tp"), None), P(None, "tp"), P("tp", None)
    return jax.shard_map(
        step,
        mesh=mesh,
        in_specs=(tokens, P(None), columns, columns, columns, rows_of, P(None), columns, columns, rows_of),
        out_specs=tokens,
        check_vma=False,
    )
```

```python
import functools

import jax
import jax.numpy as jnp
import numpy as np
from jax import lax
from jax.experimental import pallas as pl
from jax.experimental.pallas import tpu as pltpu
from jax.sharding import PartitionSpec as P

HEAD = 128
THETA = 10000
NEG = -1e30
HIDDEN = 2 * NEG
LOG2E = 1.4426950408889634
VMEM = 67_000_000
MESH = pl.DeviceIdType.MESH
PIECE = 512
WIDE = 512
GATHER_LAG = (2, 4, 5)
SHORT_LAG = (1, 2, 3)
SCATTER_LAG = (1, 3, 5)
F32, BF16 = jnp.float32, jnp.bfloat16


def _dot(a, b, ca, cb):
    return lax.dot_general(a, b, (((ca,), (cb,)), ((), ())), preferred_element_type=F32)


def _place(n):
    me = lax.axis_index("tp")
    chips = n // 2
    chip, core = me // 2, me % 2
    at = lambda step: ((chip + step) % chips) * 2 + core
    return me, core, chip * 2 + 1 - core, at(1), at(chips - 1), at(chips // 2)


def _greet(others):
    barrier = pltpu.get_barrier_semaphore()
    for other in others:
        pl.semaphore_signal(barrier, inc=1, device_id={"tp": other}, device_id_type=MESH)
    pl.semaphore_wait(barrier, len(others))


def _gather_kernel(n, count, finish, tile, lag, x_ref, gain_ref, *rest):
    weights, rest = rest[:count], rest[count:]
    extra, rest = rest[: finish.extra], rest[finish.extra :]
    outs, rest = rest[: finish.outs], rest[finish.outs :]
    xg, acc, wbuf, wsem, osem, ssem, rsem = rest
    pieces, rows, width = xg.shape
    own = rows // n
    half = own // 2
    each = weights[0].shape[1]
    me, core, partner, right, left, opposite = _place(n)

    def weight_copies(k):
        return [
            pltpu.make_async_copy(w.at[pl.ds(k * width, width), :], wbuf.at[k % 2, :, pl.ds(j * each, each)], wsem.at[k % 2, j])
            for j, w in enumerate(weights)
        ]

    for k in range(2):
        for c in weight_copies(k):
            c.start()

    def squares(k, total):
        wide = x_ref[:, pl.ds(k * width, width)].astype(F32)
        return total + jnp.sum(wide * wide, -1, keepdims=True)

    total = lax.fori_loop(0, pieces, squares, jnp.zeros((own, 1), F32))
    scale = lax.rsqrt(total * (1 / (pieces * width)) + 1e-6)
    mine = pl.multiple_of(me * own, own)

    def norm(k, _):
        here = pl.ds(k * width, width)
        xg[k, pl.ds(mine, own), :] = (x_ref[:, here].astype(F32) * scale * gain_ref[here].astype(F32)[None, :]).astype(BF16)

    lax.fori_loop(0, pieces, norm, None)
    _greet((partner, right, left))

    def copy(k, m, owner, low, size, to):
        block = xg.at[k, pl.ds(pl.multiple_of(owner * own + low, half), size), :]
        return pltpu.make_async_remote_copy(block, block, ssem.at[k, m], rsem.at[k, m], device_id={"tp": to}, device_id_type=MESH)

    across = lambda other: other + 1 - 2 * core
    opp2, left2, right2 = across(opposite), across(left), across(right)

    sent = (
        (me, 0, own, partner),
        (me, 0, own, right),
        (me, 0, own, left),
        (left, 0, half, right),
        (right, half, half, left),
        (left, 0, own, partner),
        (right, 0, own, partner),
        (opposite, 0, half, partner),
        (opposite, half, half, partner),
    )
    landed = (
        (partner, 0, own, partner),
        (left, 0, own, partner),
        (right, 0, own, partner),
        (opposite, 0, half, partner),
        (opposite, half, half, partner),
        (left2, 0, own, partner),
        (right2, 0, own, partner),
        (opp2, 0, half, partner),
        (opp2, half, half, partner),
    )

    def start(k, *which):
        for m in which:
            copy(k, m, *sent[m]).start()

    def await_(k, *which):
        for m in which:
            copy(k, m, *landed[m]).wait_recv()

    acc[...] = jnp.zeros_like(acc)

    def step(s, _):
        @pl.when(s < pieces)
        def _():
            start(s, 1, 2, 0)

        @pl.when((s >= lag[0]) & (s < pieces + lag[0]))
        def _():
            k = s - lag[0]
            await_(k, 1)
            start(k, 3, 5)
            await_(k, 2)
            start(k, 4, 6)

        @pl.when((s >= lag[1]) & (s < pieces + lag[1]))
        def _():
            k = s - lag[1]
            await_(k, 3)
            start(k, 7)
            await_(k, 4)
            start(k, 8)

        @pl.when(s >= lag[2])
        def _():
            k = s - lag[2]
            await_(k, 0, 5, 6, 7, 8)
            for c in weight_copies(k):
                c.wait()

            def columns(t, _):
                here = pl.ds(pl.multiple_of(t * tile, tile), tile)
                acc[:, here] += _dot(xg[k], wbuf[k % 2, :, here], 1, 0)

            lax.fori_loop(0, acc.shape[1] // tile, columns, None)

            @pl.when(k + 2 < pieces)
            def _():
                for c in weight_copies(k + 2):
                    c.start()

    lax.fori_loop(0, pieces + lag[2], step, None)
    finish(acc, wbuf, extra, outs, osem)

    def drain(k, _):
        for m in range(len(sent)):
            copy(k, m, *sent[m]).wait_send()

    lax.fori_loop(0, pieces, drain, None)


class _Blocks:
    def __init__(self, parts, outs, extra):
        self.parts, self.outs, self.extra = parts, outs, extra

    def __call__(self, acc, wbuf, extra, outs, osem):
        rows = wbuf.shape[1] // 2
        each = outs[0].shape[1]
        copies = []
        for b in range(acc.shape[0] // rows):
            low, first = (b % 2) * rows, 0
            for groups, values in self.parts:

                def columns(t, _):
                    at = pl.multiple_of(t * WIDE, WIDE)
                    wbuf[b // 2, low : low + rows, pl.ds(at, WIDE)] = values(acc, extra, b * rows, rows, at)

                lax.fori_loop(first, first + groups, columns, None)
                first += groups
            for j, out in enumerate(outs):
                c = pltpu.make_async_copy(
                    wbuf.at[b // 2, pl.ds(low, rows), pl.ds(j * each, each)], out.at[pl.ds(b * rows, rows), :], osem.at[b, j]
                )
                c.start()
                copies.append(c)
        for c in copies:
            c.wait()


def _gather(n, collective_id, x, gain, weights, finish, tile, lag, extra, out_columns):
    own, depth = x.shape
    rows, each, count = own * n, weights[0].shape[1], len(weights)
    pieces = depth // PIECE
    vmem, hbm = pl.BlockSpec(memory_space=pltpu.VMEM), pl.BlockSpec(memory_space=pl.ANY)
    return pl.pallas_call(
        functools.partial(_gather_kernel, n, count, finish, tile, lag),
        out_shape=[jax.ShapeDtypeStruct((rows, out_columns), BF16)] * finish.outs,
        in_specs=[vmem, vmem] + [hbm] * count + [vmem] * finish.extra,
        out_specs=[hbm] * finish.outs,
        scratch_shapes=[
            pltpu.VMEM((pieces, rows, PIECE), BF16),
            pltpu.VMEM((rows, each * count), F32),
            pltpu.VMEM((2, PIECE, each * count), BF16),
            pltpu.SemaphoreType.DMA((2, count)),
            pltpu.SemaphoreType.DMA((4, finish.outs)),
            pltpu.SemaphoreType.DMA((pieces, 9)),
            pltpu.SemaphoreType.DMA((pieces, 9)),
        ],
        compiler_params=pltpu.CompilerParams(collective_id=collective_id, has_side_effects=True, vmem_limit_bytes=VMEM),
        cost_estimate=pl.CostEstimate(
            flops=2 * rows * depth * each * count, bytes_accessed=2 * depth * each * count, transcendentals=rows * each
        ),
    )(x, gain, *weights, *extra)


def _scatter_kernel(n, lag, a_ref, w_ref, x_ref, o_ref, a_v, wbuf, keep, d_out, d_in, a_out, a_in, b_out, b_in, asem, wsem, ssem, rsem):
    pieces, width = d_in.shape[0], wbuf.shape[2]
    slots, own = keep.shape[0], keep.shape[2]
    half = own // 2
    chips = n // 2
    me, core, partner, right, left, opposite = _place(n)

    def weight_copy(k):
        here = pl.ds(pl.multiple_of(k * width, width), width)
        return pltpu.make_async_copy(w_ref.at[:, here], wbuf.at[k % 3], wsem.at[k % 3])

    fetch = pltpu.make_async_copy(a_ref, a_v, asem)
    fetch.start()
    for k in range(2):
        weight_copy(k).start()
    _greet((partner, right, left))

    def copy(k, m, source, target, to):
        return pltpu.make_async_remote_copy(source, target, ssem.at[k, m], rsem.at[k, m], device_id={"tp": to}, device_id_type=MESH)

    def cores(k):
        return copy(k, 0, d_out.at[k % 2], d_in.at[k], partner)

    def far(k):
        return [
            copy(k, 1, a_out.at[k % 2, pl.ds(0, half)], a_in.at[k, pl.ds(0, half)], right),
            copy(k, 2, a_out.at[k % 2, pl.ds(half, half)], a_in.at[k, pl.ds(half, half)], left),
        ]

    def near(k):
        return [copy(k, 3, b_out.at[k % 2, 0], b_in.at[k, 0], right), copy(k, 4, b_out.at[k % 2, 1], b_in.at[k, 1], left)]

    def term(k, owner, low=0, size=own):
        here = pl.ds(low, size)
        return keep[k % slots, owner, here, :] + d_in[k, owner // 2, here, :].astype(F32)

    fetch.wait()

    def step(s, _):
        @pl.when(s < pieces)
        def _():
            weight_copy(s).wait()

            @pl.when(s + 2 < pieces)
            def _():
                weight_copy(s + 2).start()

            keep[s % slots] = _dot(a_v[...], wbuf[s % 3], 1, 0).reshape(n, own, width)

            @pl.when(s >= 2)
            def _():
                cores(s - 2).wait_send()

            for q in range(chips):
                d_out[s % 2, q] = keep[s % slots, 2 * q + 1 - core].astype(BF16)

        @pl.when((s >= lag[0]) & (s < pieces + lag[0]))
        def _():
            k = s - lag[0]
            cores(k).wait_recv()

            @pl.when(k >= 2)
            def _():
                for c in far(k - 2):
                    c.wait_send()

            a_out[k % 2] = term(k, opposite).astype(BF16)

        @pl.when(s < pieces)
        def _():
            cores(s).start()

        @pl.when((s >= lag[1]) & (s < pieces + lag[1]))
        def _():
            k = s - lag[1]
            for c in far(k):
                c.wait_recv()

            @pl.when(k >= 2)
            def _():
                for c in near(k - 2):
                    c.wait_send()

            b_out[k % 2, 0, pl.ds(0, half)] = (term(k, right, 0, half) + a_in[k, pl.ds(0, half)].astype(F32)).astype(BF16)
            b_out[k % 2, 0, pl.ds(half, half)] = term(k, right, half, half).astype(BF16)
            b_out[k % 2, 1, pl.ds(0, half)] = term(k, left, 0, half).astype(BF16)
            b_out[k % 2, 1, pl.ds(half, half)] = (term(k, left, half, half) + a_in[k, pl.ds(half, half)].astype(F32)).astype(BF16)

        @pl.when((s >= lag[0]) & (s < pieces + lag[0]))
        def _():
            for c in far(s - lag[0]):
                c.start()

        @pl.when(s >= lag[2])
        def _():
            k = s - lag[2]
            for c in near(k):
                c.wait_recv()
            here = pl.ds(pl.multiple_of(k * width, width), width)
            total = term(k, me) + b_in[k, 0].astype(F32) + b_in[k, 1].astype(F32)
            o_ref[:, here] = (x_ref[:, here].astype(F32) + total).astype(BF16)

        @pl.when((s >= lag[1]) & (s < pieces + lag[1]))
        def _():
            for c in near(s - lag[1]):
                c.start()

    lax.fori_loop(0, pieces + lag[2], step, None)
    for k in (pieces - 2, pieces - 1):
        for c in [cores(k), *far(k), *near(k)]:
            c.wait_send()


def _scatter(n, collective_id, a, w, x):
    rows, depth = a.shape
    own, columns = x.shape
    pieces = columns // PIECE
    vmem, hbm = pl.BlockSpec(memory_space=pltpu.VMEM), pl.BlockSpec(memory_space=pl.ANY)
    return pl.pallas_call(
        functools.partial(_scatter_kernel, n, SCATTER_LAG),
        out_shape=jax.ShapeDtypeStruct((own, columns), BF16),
        in_specs=[hbm, hbm, vmem],
        out_specs=vmem,
        scratch_shapes=[
            pltpu.VMEM((rows, depth), BF16),
            pltpu.VMEM((3, depth, PIECE), BF16),
            pltpu.VMEM((SCATTER_LAG[2] + 1, n, own, PIECE), F32),
            pltpu.VMEM((2, n // 2, own, PIECE), BF16),
            pltpu.VMEM((pieces, n // 2, own, PIECE), BF16),
            pltpu.VMEM((2, own, PIECE), BF16),
            pltpu.VMEM((pieces, own, PIECE), BF16),
            pltpu.VMEM((2, 2, own, PIECE), BF16),
            pltpu.VMEM((pieces, 2, own, PIECE), BF16),
            pltpu.SemaphoreType.DMA,
            pltpu.SemaphoreType.DMA((3,)),
            pltpu.SemaphoreType.DMA((pieces, 5)),
            pltpu.SemaphoreType.DMA((pieces, 5)),
        ],
        compiler_params=pltpu.CompilerParams(collective_id=collective_id, has_side_effects=True, vmem_limit_bytes=VMEM),
        cost_estimate=pl.CostEstimate(flops=2 * rows * depth * columns, bytes_accessed=2 * depth * columns, transcendentals=0),
    )(a, w, x)


def _attention_kernel(q_ref, k_ref, v_ref, o_ref, top_s, mix_s, *, bq, bk, scale):
    heads = top_s.shape[0]
    iq = pl.program_id(0)
    e = scale * LOG2E
    top_s[...] = jnp.full(top_s.shape, NEG, F32)
    mix_s[...] = jnp.zeros(mix_s.shape, F32)
    ones = jnp.ones((8, bk), BF16)
    gap = lax.broadcasted_iota(jnp.int32, (bk, bq), 1) - lax.broadcasted_iota(jnp.int32, (bk, bq), 0)
    part = lambda i: slice(i * HEAD, (i + 1) * HEAD)

    def block(j, masked):
        here = pl.ds(pl.multiple_of(j * bk, bk), bk)
        scores = [_dot(k_ref[here, part(i)], q_ref[:, part(i)], 1, 1) for i in range(heads)]
        weights, keeps = [], []
        for i, s in enumerate(scores):
            if masked:
                s = jnp.where(gap >= j * bk - iq * bq, s, HIDDEN)
            old = top_s[i : i + 1, :]
            top = jnp.maximum(old, s.max(axis=0, keepdims=True))
            top_s[i : i + 1, :] = top
            weights.append(jnp.exp2((s - top) * e).astype(BF16))
            keeps.append(jnp.exp2((old - top) * e))
        for i, (p, keep) in enumerate(zip(weights, keeps)):
            values = jnp.concatenate([v_ref[here, part(i)].T, ones], axis=0)
            mix_s[i] = mix_s[i] * keep + _dot(values, p, 1, 0)

    whole = iq * bq // bk
    lax.fori_loop(0, whole, lambda j, _: block(j, False), None)
    lax.fori_loop(whole, whole + bq // bk, lambda j, _: block(j, True), None)
    for i in range(heads):
        total = mix_s[i, HEAD : HEAD + 1, :]
        o_ref[:, part(i)] = (mix_s[i, :HEAD, :] * (1 / total)).T.astype(BF16)


def _attention(q, k, v, bq=256, bk=256):
    rows, columns = q.shape
    heads = columns // HEAD
    some = pl.BlockSpec((bq, columns), lambda i: (i, 0))
    every = pl.BlockSpec((rows, columns), lambda i: (0, 0))
    return pl.pallas_call(
        functools.partial(_attention_kernel, bq=bq, bk=bk, scale=HEAD**-0.5),
        grid=(rows // bq,),
        in_specs=[some, every, every],
        out_specs=some,
        out_shape=jax.ShapeDtypeStruct((rows, columns), BF16),
        scratch_shapes=[pltpu.VMEM((heads, bq), F32), pltpu.VMEM((heads, HEAD + 8, bq), F32)],
        compiler_params=pltpu.CompilerParams(dimension_semantics=("arbitrary",), vmem_limit_bytes=56 * 2**20),
        cost_estimate=pl.CostEstimate(flops=4 * rows * rows * columns, bytes_accessed=8 * rows * columns, transcendentals=heads * rows * rows),
    )(q, k, v)


def _tables(rows):
    half = HEAD // 2
    rate = (np.float32(THETA) ** (-np.arange(half, dtype=np.float32) / np.float32(half))).astype(np.float32)
    angle = np.arange(rows, dtype=np.float32)[:, None] * rate
    cos, sin = np.cos(angle.astype(np.float64)), np.sin(angle.astype(np.float64))
    return np.concatenate([cos, cos], 1).astype(np.float32), np.concatenate([-sin, sin], 1).astype(np.float32)


def _turned(acc, extra, low, rows, at):
    cos, sin = (r[low : low + rows, :] for r in extra)
    heads = []
    for i in range(0, WIDE, HEAD):
        wide = acc[low : low + rows, pl.ds(at + i, HEAD)].astype(BF16).astype(F32)
        heads.append((wide * cos + pltpu.roll(wide, HEAD // 2, 1) * sin).astype(BF16))
    return jnp.concatenate(heads, 1)


def _plain(acc, extra, low, rows, at):
    return acc[low : low + rows, pl.ds(at, WIDE)].astype(BF16)


def _hidden(acc, extra, low, rows, at):
    gate = acc[low : low + rows, pl.ds(at, WIDE)]
    up = acc[low : low + rows, pl.ds(at + acc.shape[1] // 2, WIDE)]
    return (gate * lax.logistic(gate) * up).astype(BF16)


def solution(mesh):
    n = mesh.shape["tp"]

    def step(x, gain_a, wq, wk, wv, wo, gain_m, w_gate, w_up, w_down):
        rows = x.shape[0] * n
        tables = [jnp.asarray(t) for t in _tables(rows)]
        q, k, v = _gather(n, 0, x, gain_a, (wq, wk, wv), _Blocks([(2 * wq.shape[1] // WIDE, _turned), (wv.shape[1] // WIDE, _plain)], 3, 2), 3072, GATHER_LAG, tables, wq.shape[1])
        seen = _attention(q, k, v)
        h = _scatter(n, 1, seen, wo, x)
        (hidden,) = _gather(n, 2, h, gain_m, (w_gate, w_up), _Blocks([(w_gate.shape[1] // WIDE, _hidden)], 1, 0), 2048, SHORT_LAG, (), w_gate.shape[1])
        return _scatter(n, 3, hidden, w_down, h)

    tokens, columns, rows_of = P(("dp", "tp"), None), P(None, "tp"), P("tp", None)
    return jax.shard_map(
        step,
        mesh=mesh,
        in_specs=(tokens, P(None), columns, columns, columns, rows_of, P(None), columns, columns, rows_of),
        out_specs=tokens,
        check_vma=False,
    )
```

```python
import functools

import jax
import jax.numpy as jnp
import numpy as np
from jax import lax
from jax.experimental import pallas as pl
from jax.experimental.pallas import tpu as pltpu
from jax.sharding import PartitionSpec as P

HEAD = 128
THETA = 10000
NEG = -1e30
HIDDEN = 2 * NEG
LOG2E = 1.4426950408889634
VMEM = 67_000_000
MESH = pl.DeviceIdType.MESH
PIECE = 512
WIDE = 512
GATHER_LAG = (2, 4, 5)
SHORT_LAG = (1, 2, 3)
SCATTER_LAG = (1, 3, 5)
F32, BF16 = jnp.float32, jnp.bfloat16


def _dot(a, b, ca, cb):
    return lax.dot_general(a, b, (((ca,), (cb,)), ((), ())), preferred_element_type=F32)


def _place(n):
    me = lax.axis_index("tp")
    chips = n // 2
    chip, core = me // 2, me % 2
    at = lambda step: ((chip + step) % chips) * 2 + core
    return me, core, chip * 2 + 1 - core, at(1), at(chips - 1), at(chips // 2)


def _greet(others):
    barrier = pltpu.get_barrier_semaphore()
    for other in others:
        pl.semaphore_signal(barrier, inc=1, device_id={"tp": other}, device_id_type=MESH)
    return lambda: pl.semaphore_wait(barrier, len(others))


def _gather_kernel(n, count, finish, tile, lag, x_ref, gain_ref, *rest):
    weights, rest = rest[:count], rest[count:]
    extra, rest = rest[: finish.extra], rest[finish.extra :]
    outs, rest = rest[: finish.outs], rest[finish.outs :]
    xg, acc, wbuf, wsem, osem, ssem, rsem = rest
    pieces, rows, width = xg.shape
    own = rows // n
    half = own // 2
    each = weights[0].shape[1]
    me, core, partner, right, left, opposite = _place(n)

    def weight_copies(k):
        return [
            pltpu.make_async_copy(w.at[pl.ds(k * width, width), :], wbuf.at[k % 2, :, pl.ds(j * each, each)], wsem.at[k % 2, j])
            for j, w in enumerate(weights)
        ]

    for k in range(2):
        for c in weight_copies(k):
            c.start()

    met = _greet((partner, right, left))

    def squares(k, total):
        wide = x_ref[:, pl.ds(k * width, width)].astype(F32)
        return total + jnp.sum(wide * wide, -1, keepdims=True)

    total = lax.fori_loop(0, pieces, squares, jnp.zeros((own, 1), F32))
    scale = lax.rsqrt(total * (1 / (pieces * width)) + 1e-6)
    mine = pl.multiple_of(me * own, own)

    def norm(k, _):
        here = pl.ds(k * width, width)
        xg[k, pl.ds(mine, own), :] = (x_ref[:, here].astype(F32) * scale * gain_ref[here].astype(F32)[None, :]).astype(BF16)

    lax.fori_loop(0, 2, norm, None)
    def copy(k, m, owner, low, size, to):
        block = xg.at[k, pl.ds(pl.multiple_of(owner * own + low, half), size), :]
        return pltpu.make_async_remote_copy(block, block, ssem.at[k, m], rsem.at[k, m], device_id={"tp": to}, device_id_type=MESH)

    across = lambda other: other + 1 - 2 * core
    opp2, left2, right2 = across(opposite), across(left), across(right)

    sent = (
        (me, 0, own, partner),
        (me, 0, own, right),
        (me, 0, own, left),
        (left, 0, half, right),
        (right, half, half, left),
        (left, 0, own, partner),
        (right, 0, own, partner),
        (opposite, 0, half, partner),
        (opposite, half, half, partner),
    )
    landed = (
        (partner, 0, own, partner),
        (left, 0, own, partner),
        (right, 0, own, partner),
        (opposite, 0, half, partner),
        (opposite, half, half, partner),
        (left2, 0, own, partner),
        (right2, 0, own, partner),
        (opp2, 0, half, partner),
        (opp2, half, half, partner),
    )

    def start(k, *which):
        for m in which:
            copy(k, m, *sent[m]).start()

    def await_(k, *which):
        for m in which:
            copy(k, m, *landed[m]).wait_recv()

    met()
    for k in range(2):
        start(k, 1, 2, 0)
    lax.fori_loop(2, pieces, norm, None)
    acc[...] = jnp.zeros_like(acc)

    def step(s, _):
        @pl.when((s >= 2) & (s < pieces))
        def _():
            start(s, 1, 2, 0)

        @pl.when((s >= lag[0]) & (s < pieces + lag[0]))
        def _():
            k = s - lag[0]
            await_(k, 1)
            start(k, 3, 5)
            await_(k, 2)
            start(k, 4, 6)

        @pl.when((s >= lag[1]) & (s < pieces + lag[1]))
        def _():
            k = s - lag[1]
            await_(k, 3)
            start(k, 7)
            await_(k, 4)
            start(k, 8)

        @pl.when(s >= lag[2])
        def _():
            k = s - lag[2]
            await_(k, 0, 5, 6, 7, 8)
            for c in weight_copies(k):
                c.wait()

            def columns(t, _):
                here = pl.ds(pl.multiple_of(t * tile, tile), tile)
                acc[:, here] += _dot(xg[k], wbuf[k % 2, :, here], 1, 0)

            lax.fori_loop(0, acc.shape[1] // tile, columns, None)

            @pl.when(k + 2 < pieces)
            def _():
                for c in weight_copies(k + 2):
                    c.start()

    lax.fori_loop(0, pieces + lag[2], step, None)
    finish(acc, wbuf, extra, outs, osem)

    def drain(k, _):
        for m in range(len(sent)):
            copy(k, m, *sent[m]).wait_send()

    lax.fori_loop(0, pieces, drain, None)


class _Blocks:
    def __init__(self, parts, outs, extra):
        self.parts, self.outs, self.extra = parts, outs, extra

    def __call__(self, acc, wbuf, extra, outs, osem):
        rows = wbuf.shape[1] // 2
        each = outs[0].shape[1]
        copies = []
        for b in range(acc.shape[0] // rows):
            low, first = (b % 2) * rows, 0
            for groups, values in self.parts:

                def columns(t, _):
                    at = pl.multiple_of(t * WIDE, WIDE)
                    wbuf[b // 2, low : low + rows, pl.ds(at, WIDE)] = values(acc, extra, b * rows, rows, at)

                lax.fori_loop(first, first + groups, columns, None)
                first += groups
            for j, out in enumerate(outs):
                c = pltpu.make_async_copy(
                    wbuf.at[b // 2, pl.ds(low, rows), pl.ds(j * each, each)], out.at[pl.ds(b * rows, rows), :], osem.at[b, j]
                )
                c.start()
                copies.append(c)
        for c in copies:
            c.wait()


def _gather(n, collective_id, x, gain, weights, finish, tile, lag, extra, out_columns):
    own, depth = x.shape
    rows, each, count = own * n, weights[0].shape[1], len(weights)
    pieces = depth // PIECE
    vmem, hbm = pl.BlockSpec(memory_space=pltpu.VMEM), pl.BlockSpec(memory_space=pl.ANY)
    return pl.pallas_call(
        functools.partial(_gather_kernel, n, count, finish, tile, lag),
        out_shape=[jax.ShapeDtypeStruct((rows, out_columns), BF16)] * finish.outs,
        in_specs=[vmem, vmem] + [hbm] * count + [vmem] * finish.extra,
        out_specs=[hbm] * finish.outs,
        scratch_shapes=[
            pltpu.VMEM((pieces, rows, PIECE), BF16),
            pltpu.VMEM((rows, each * count), F32),
            pltpu.VMEM((2, PIECE, each * count), BF16),
            pltpu.SemaphoreType.DMA((2, count)),
            pltpu.SemaphoreType.DMA((4, finish.outs)),
            pltpu.SemaphoreType.DMA((pieces, 9)),
            pltpu.SemaphoreType.DMA((pieces, 9)),
        ],
        compiler_params=pltpu.CompilerParams(collective_id=collective_id, has_side_effects=True, vmem_limit_bytes=VMEM),
        cost_estimate=pl.CostEstimate(
            flops=2 * rows * depth * each * count, bytes_accessed=2 * depth * each * count, transcendentals=rows * each
        ),
    )(x, gain, *weights, *extra)


def _scatter_kernel(n, lag, a_ref, w_ref, x_ref, o_ref, a_v, wbuf, keep, d_out, d_in, a_out, a_in, b_out, b_in, asem, wsem, ssem, rsem):
    pieces, width = d_in.shape[0], wbuf.shape[2]
    slots, own = keep.shape[0], keep.shape[2]
    half = own // 2
    chips = n // 2
    me, core, partner, right, left, opposite = _place(n)

    def weight_copy(k):
        here = pl.ds(pl.multiple_of(k * width, width), width)
        return pltpu.make_async_copy(w_ref.at[:, here], wbuf.at[k % 3], wsem.at[k % 3])

    fetch = pltpu.make_async_copy(a_ref, a_v, asem)
    fetch.start()
    for k in range(2):
        weight_copy(k).start()
    met = _greet((partner, right, left))

    def copy(k, m, source, target, to):
        return pltpu.make_async_remote_copy(source, target, ssem.at[k, m], rsem.at[k, m], device_id={"tp": to}, device_id_type=MESH)

    def cores(k):
        return copy(k, 0, d_out.at[k % 2], d_in.at[k], partner)

    def far(k):
        return [
            copy(k, 1, a_out.at[k % 2, pl.ds(0, half)], a_in.at[k, pl.ds(0, half)], right),
            copy(k, 2, a_out.at[k % 2, pl.ds(half, half)], a_in.at[k, pl.ds(half, half)], left),
        ]

    def near(k):
        return [copy(k, 3, b_out.at[k % 2, 0], b_in.at[k, 0], right), copy(k, 4, b_out.at[k % 2, 1], b_in.at[k, 1], left)]

    def term(k, owner, low=0, size=own):
        here = pl.ds(low, size)
        return keep[k % slots, owner, here, :] + d_in[k, owner // 2, here, :].astype(F32)

    fetch.wait()
    met()

    def step(s, _):
        @pl.when(s < pieces)
        def _():
            weight_copy(s).wait()

            @pl.when(s + 2 < pieces)
            def _():
                weight_copy(s + 2).start()

            keep[s % slots] = _dot(a_v[...], wbuf[s % 3], 1, 0).reshape(n, own, width)

            @pl.when(s >= 2)
            def _():
                cores(s - 2).wait_send()

            for q in range(chips):
                d_out[s % 2, q] = keep[s % slots, 2 * q + 1 - core].astype(BF16)

        @pl.when((s >= lag[0]) & (s < pieces + lag[0]))
        def _():
            k = s - lag[0]
            cores(k).wait_recv()

            @pl.when(k >= 2)
            def _():
                for c in far(k - 2):
                    c.wait_send()

            a_out[k % 2] = term(k, opposite).astype(BF16)

        @pl.when(s < pieces)
        def _():
            cores(s).start()

        @pl.when((s >= lag[1]) & (s < pieces + lag[1]))
        def _():
            k = s - lag[1]
            for c in far(k):
                c.wait_recv()

            @pl.when(k >= 2)
            def _():
                for c in near(k - 2):
                    c.wait_send()

            b_out[k % 2, 0, pl.ds(0, half)] = (term(k, right, 0, half) + a_in[k, pl.ds(0, half)].astype(F32)).astype(BF16)
            b_out[k % 2, 0, pl.ds(half, half)] = term(k, right, half, half).astype(BF16)
            b_out[k % 2, 1, pl.ds(0, half)] = term(k, left, 0, half).astype(BF16)
            b_out[k % 2, 1, pl.ds(half, half)] = (term(k, left, half, half) + a_in[k, pl.ds(half, half)].astype(F32)).astype(BF16)

        @pl.when((s >= lag[0]) & (s < pieces + lag[0]))
        def _():
            for c in far(s - lag[0]):
                c.start()

        @pl.when(s >= lag[2])
        def _():
            k = s - lag[2]
            for c in near(k):
                c.wait_recv()
            here = pl.ds(pl.multiple_of(k * width, width), width)
            total = term(k, me) + b_in[k, 0].astype(F32) + b_in[k, 1].astype(F32)
            o_ref[:, here] = (x_ref[:, here].astype(F32) + total).astype(BF16)

        @pl.when((s >= lag[1]) & (s < pieces + lag[1]))
        def _():
            for c in near(s - lag[1]):
                c.start()

    lax.fori_loop(0, pieces + lag[2], step, None)
    for k in (pieces - 2, pieces - 1):
        for c in [cores(k), *far(k), *near(k)]:
            c.wait_send()


def _scatter(n, collective_id, a, w, x):
    rows, depth = a.shape
    own, columns = x.shape
    pieces = columns // PIECE
    vmem, hbm = pl.BlockSpec(memory_space=pltpu.VMEM), pl.BlockSpec(memory_space=pl.ANY)
    return pl.pallas_call(
        functools.partial(_scatter_kernel, n, SCATTER_LAG),
        out_shape=jax.ShapeDtypeStruct((own, columns), BF16),
        in_specs=[hbm, hbm, vmem],
        out_specs=vmem,
        scratch_shapes=[
            pltpu.VMEM((rows, depth), BF16),
            pltpu.VMEM((3, depth, PIECE), BF16),
            pltpu.VMEM((SCATTER_LAG[2] + 1, n, own, PIECE), F32),
            pltpu.VMEM((2, n // 2, own, PIECE), BF16),
            pltpu.VMEM((pieces, n // 2, own, PIECE), BF16),
            pltpu.VMEM((2, own, PIECE), BF16),
            pltpu.VMEM((pieces, own, PIECE), BF16),
            pltpu.VMEM((2, 2, own, PIECE), BF16),
            pltpu.VMEM((pieces, 2, own, PIECE), BF16),
            pltpu.SemaphoreType.DMA,
            pltpu.SemaphoreType.DMA((3,)),
            pltpu.SemaphoreType.DMA((pieces, 5)),
            pltpu.SemaphoreType.DMA((pieces, 5)),
        ],
        compiler_params=pltpu.CompilerParams(collective_id=collective_id, has_side_effects=True, vmem_limit_bytes=VMEM),
        cost_estimate=pl.CostEstimate(flops=2 * rows * depth * columns, bytes_accessed=2 * depth * columns, transcendentals=0),
    )(a, w, x)


def _attend_kernel(n, bk, scale, q_ref, k_ref, v_ref, w_ref, x_ref, o_ref, q_v, k_v, v_v, w_v, seen, top_s, mix_s, keep, d_out, d_in,
                   a_out, a_in, b_in, lsem, wsem, dsend, drecv, ssem, rsem):
    heads = top_s.shape[0]
    pieces, own, width = a_in.shape
    half, both = own // 2, 2 * own
    me, core, partner, right, left, opposite = _place(n)
    order = (opposite // 2, right // 2, left // 2, me // 2)

    fetches = [pltpu.make_async_copy(r, t, lsem.at[i]) for i, (r, t) in enumerate(((k_ref, k_v), (v_ref, v_v)))]
    queries = [
        pltpu.make_async_copy(q_ref.at[pl.ds(pl.multiple_of(c * both, both), both), :], q_v.at[i], lsem.at[2 + i])
        for i, c in enumerate(order)
    ]
    for c in queries[:1] + fetches:
        c.start()

    def weight_copy(j):
        return pltpu.make_async_copy(w_ref.at[:, pl.ds(pl.multiple_of(j * width, width), width)], w_v.at[j], wsem.at[j])

    def loop(f):
        lax.fori_loop(0, pieces, lambda j, _: f(j), None)

    loop(lambda j: weight_copy(j).start())
    for c in queries[1:]:
        c.start()
    met = _greet((partner, right, left))
    for c in fetches:
        c.wait()

    e = scale * LOG2E
    ones = jnp.ones((8, bk), BF16)
    gap = lax.broadcasted_iota(jnp.int32, (bk, both), 1) - lax.broadcasted_iota(jnp.int32, (bk, both), 0)
    part = lambda i: slice(i * HEAD, (i + 1) * HEAD)

    def attend(stage):
        chip = order[stage]
        queries[stage].wait()
        top_s[...] = jnp.full(top_s.shape, NEG, F32)
        mix_s[...] = jnp.zeros(mix_s.shape, F32)

        def block(j, masked):
            here = pl.ds(pl.multiple_of(j * bk, bk), bk)
            scores = [_dot(k_v[here, part(i)], q_v[stage, :, part(i)], 1, 1) for i in range(heads)]
            weights, keeps = [], []
            for i, s in enumerate(scores):
                if masked:
                    s = jnp.where(gap >= j * bk - chip * both, s, HIDDEN)
                old = top_s[i : i + 1, :]
                top = jnp.maximum(old, s.max(axis=0, keepdims=True))
                top_s[i : i + 1, :] = top
                weights.append(jnp.exp2((s - top) * e).astype(BF16))
                keeps.append(jnp.exp2((old - top) * e))
            for i, (p, keep_) in enumerate(zip(weights, keeps)):
                values = jnp.concatenate([v_v[here, part(i)].T, ones], axis=0)
                mix_s[i] = mix_s[i] * keep_ + _dot(values, p, 1, 0)

        whole = chip * (both // bk)
        lax.fori_loop(0, whole, lambda j, _: block(j, False), None)
        lax.fori_loop(whole, whole + both // bk, lambda j, _: block(j, True), None)
        for i in range(heads):
            total = mix_s[i, HEAD : HEAD + 1, :]
            seen[:, part(i)] = (mix_s[i, :HEAD, :] * (1 / total)).T.astype(BF16)

    def d_target(stage, j):
        return a_out.at[j] if stage == 3 else d_out.at[stage % 2, j]

    def cores(stage, j):
        return pltpu.make_async_remote_copy(
            d_target(stage, j), d_in.at[stage, j], dsend.at[stage, j], drecv.at[stage, j], device_id={"tp": partner}, device_id_type=MESH
        )

    def copy(j, m, source, target, to):
        return pltpu.make_async_remote_copy(source, target, ssem.at[j, m], rsem.at[j, m], device_id={"tp": to}, device_id_type=MESH)

    low, high = pl.ds(0, half), pl.ds(half, half)

    def far(j):
        return [copy(j, 0, a_out.at[j, low], a_in.at[j, low], right), copy(j, 1, a_out.at[j, high], a_in.at[j, high], left)]

    def near(j, side):
        return copy(j, 2 + side, d_out.at[side, j], b_in.at[j, side], (right, left)[side])

    def term(stage, j, rows):
        return keep[stage % 3, j, rows, :] + d_in[stage, j, rows, :].astype(F32)

    def multiply(stage, j):
        both_rows = _dot(seen[...], w_v[j], 1, 0).reshape(2, own, width)
        mix = jnp.where(core == 0, both_rows[0], both_rows[1])
        keep[stage % 3, j] = mix
        d_target(stage, j)[...] = jnp.where(core == 0, both_rows[1], both_rows[0]).astype(BF16)

    every = pl.ds(0, own)

    def first(j):
        cores(0, j).wait_recv()
        a_out[j] = term(0, j, every).astype(BF16)

    attend(0)
    met()

    def opening(j, _):
        @pl.when(j < pieces)
        def _():
            weight_copy(j).wait()
            multiply(0, j)

        @pl.when((j >= 2) & (j < pieces + 2))
        def _():
            first(j - 2)

        @pl.when(j < pieces)
        def _():
            cores(0, j).start()

        @pl.when(j >= 3)
        def _():
            for c in far(j - 3):
                c.start()

    lax.fori_loop(0, pieces + 3, opening, None)

    def terms(stage):
        attend(stage)

        def term_piece(j, _):
            @pl.when(j < pieces)
            def _():
                if stage == 2:
                    cores(0, j).wait_send()
                if stage == 3:
                    for c in far(j):
                        c.wait_send()
                multiply(stage, j)

            @pl.when(j >= 1)
            def _():
                cores(stage, j - 1).start()

        lax.fori_loop(0, pieces + 1, term_piece, None)

    def second(j, _):
        @pl.when(j < pieces)
        def _():
            for c in far(j):
                c.wait_recv()
            cores(1, j).wait_recv()
            cores(2, j).wait_recv()
            cores(1, j).wait_send()
            cores(2, j).wait_send()
            d_out[0, j, low] = (term(1, j, low) + a_in[j, low].astype(F32)).astype(BF16)
            d_out[0, j, high] = term(1, j, high).astype(BF16)
            d_out[1, j, low] = term(2, j, low).astype(BF16)
            d_out[1, j, high] = (term(2, j, high) + a_in[j, high].astype(F32)).astype(BF16)

        @pl.when(j >= 1)
        def _():
            near(j - 1, 0).start()
            near(j - 1, 1).start()

    terms(1)
    terms(2)
    lax.fori_loop(0, pieces + 1, second, None)
    terms(3)

    def third(j):
        cores(3, j).wait_recv()
        near(j, 0).wait_recv()
        near(j, 1).wait_recv()
        here = pl.ds(pl.multiple_of(j * width, width), width)
        total = term(3, j, every) + b_in[j, 0].astype(F32) + b_in[j, 1].astype(F32)
        o_ref[:, here] = (x_ref[:, here].astype(F32) + total).astype(BF16)

    loop(third)

    def drain(j):
        for c in (cores(3, j), near(j, 0), near(j, 1)):
            c.wait_send()

    loop(drain)


def _attend(n, collective_id, q, k, v, w, x, bk=256, width=1024):
    rows, depth = q.shape
    own, columns = x.shape
    pieces, heads, both = columns // width, depth // HEAD, 2 * own
    vmem, hbm = pl.BlockSpec(memory_space=pltpu.VMEM), pl.BlockSpec(memory_space=pl.ANY)
    return pl.pallas_call(
        functools.partial(_attend_kernel, n, bk, HEAD**-0.5),
        out_shape=jax.ShapeDtypeStruct((own, columns), BF16),
        in_specs=[hbm, hbm, hbm, hbm, vmem],
        out_specs=vmem,
        scratch_shapes=[
            pltpu.VMEM((n // 2, both, depth), BF16),
            pltpu.VMEM((rows, depth), BF16),
            pltpu.VMEM((rows, depth), BF16),
            pltpu.VMEM((pieces, depth, width), BF16),
            pltpu.VMEM((both, depth), BF16),
            pltpu.VMEM((heads, both), F32),
            pltpu.VMEM((heads, HEAD + 8, both), F32),
            pltpu.VMEM((3, pieces, own, width), F32),
            pltpu.VMEM((2, pieces, own, width), BF16),
            pltpu.VMEM((n // 2, pieces, own, width), BF16),
            pltpu.VMEM((pieces, own, width), BF16),
            pltpu.VMEM((pieces, own, width), BF16),
            pltpu.VMEM((pieces, 2, own, width), BF16),
            pltpu.SemaphoreType.DMA((2 + n // 2,)),
            pltpu.SemaphoreType.DMA((pieces,)),
            pltpu.SemaphoreType.DMA((n // 2, pieces)),
            pltpu.SemaphoreType.DMA((n // 2, pieces)),
            pltpu.SemaphoreType.DMA((pieces, 4)),
            pltpu.SemaphoreType.DMA((pieces, 4)),
        ],
        compiler_params=pltpu.CompilerParams(collective_id=collective_id, has_side_effects=True, vmem_limit_bytes=VMEM),
        cost_estimate=pl.CostEstimate(
            flops=4 * rows * rows * depth + 2 * rows * depth * columns, bytes_accessed=2 * depth * columns, transcendentals=heads * rows * rows
        ),
    )(q, k, v, w, x)


def _tables(rows):
    half = HEAD // 2
    rate = (np.float32(THETA) ** (-np.arange(half, dtype=np.float32) / np.float32(half))).astype(np.float32)
    angle = np.arange(rows, dtype=np.float32)[:, None] * rate
    cos, sin = np.cos(angle.astype(np.float64)), np.sin(angle.astype(np.float64))
    return np.concatenate([cos, cos], 1).astype(np.float32), np.concatenate([-sin, sin], 1).astype(np.float32)


def _turned(acc, extra, low, rows, at):
    cos, sin = (r[low : low + rows, :] for r in extra)
    heads = []
    for i in range(0, WIDE, HEAD):
        wide = acc[low : low + rows, pl.ds(at + i, HEAD)].astype(BF16).astype(F32)
        heads.append((wide * cos + pltpu.roll(wide, HEAD // 2, 1) * sin).astype(BF16))
    return jnp.concatenate(heads, 1)


def _plain(acc, extra, low, rows, at):
    return acc[low : low + rows, pl.ds(at, WIDE)].astype(BF16)


def _hidden(acc, extra, low, rows, at):
    gate = acc[low : low + rows, pl.ds(at, WIDE)]
    up = acc[low : low + rows, pl.ds(at + acc.shape[1] // 2, WIDE)]
    return (gate * lax.logistic(gate) * up).astype(BF16)


def solution(mesh):
    n = mesh.shape["tp"]

    def step(x, gain_a, wq, wk, wv, wo, gain_m, w_gate, w_up, w_down):
        rows = x.shape[0] * n
        tables = [jnp.asarray(t) for t in _tables(rows)]
        q, k, v = _gather(n, 0, x, gain_a, (wq, wk, wv), _Blocks([(2 * wq.shape[1] // WIDE, _turned), (wv.shape[1] // WIDE, _plain)], 3, 2), 3072, GATHER_LAG, tables, wq.shape[1])
        h = _attend(n, 1, q, k, v, wo, x)
        (hidden,) = _gather(n, 2, h, gain_m, (w_gate, w_up), _Blocks([(w_gate.shape[1] // WIDE, _hidden)], 1, 0), 2048, SHORT_LAG, (), w_gate.shape[1])
        return _scatter(n, 3, hidden, w_down, h)

    tokens, columns, rows_of = P(("dp", "tp"), None), P(None, "tp"), P("tp", None)
    return jax.shard_map(
        step,
        mesh=mesh,
        in_specs=(tokens, P(None), columns, columns, columns, rows_of, P(None), columns, columns, rows_of),
        out_specs=tokens,
        check_vma=False,
    )
```

```python
import functools

import jax
import jax.numpy as jnp
import numpy as np
from jax import lax
from jax.experimental import pallas as pl
from jax.experimental.pallas import tpu as pltpu
from jax.sharding import PartitionSpec as P

HEAD = 128
THETA = 10000
NEG = -1e30
HIDDEN = 2 * NEG
LOG2E = 1.4426950408889634
VMEM = 67_000_000
MESH = pl.DeviceIdType.MESH
PIECE = 512
WIDE = 512
GATHER_LAG = (2, 3, 4)
SHORT_LAG = (1, 2, 3)
SCATTER_LAG = (1, 2, 4)
F32, BF16 = jnp.float32, jnp.bfloat16


def _dot(a, b, ca, cb):
    return lax.dot_general(a, b, (((ca,), (cb,)), ((), ())), preferred_element_type=F32)


def _place(n):
    me = lax.axis_index("tp")
    chips = n // 2
    chip, core = me // 2, me % 2
    at = lambda step: ((chip + step) % chips) * 2 + core
    return me, core, chip * 2 + 1 - core, at(1), at(chips - 1), at(chips // 2)


def _greet(others):
    barrier = pltpu.get_barrier_semaphore()
    for other in others:
        pl.semaphore_signal(barrier, inc=1, device_id={"tp": other}, device_id_type=MESH)
    return lambda: pl.semaphore_wait(barrier, len(others))


def _gather_kernel(n, count, finish, tile, lag, x_ref, gain_ref, *rest):
    weights, rest = rest[:count], rest[count:]
    extra, rest = rest[: finish.extra], rest[finish.extra :]
    outs, rest = rest[: finish.outs], rest[finish.outs :]
    xg, acc, wbuf, wsem, osem, ssem, rsem = rest
    pieces, rows, width = xg.shape
    own = rows // n
    half = own // 2
    each = weights[0].shape[1]
    me, core, partner, right, left, opposite = _place(n)

    def weight_copies(k):
        return [
            pltpu.make_async_copy(w.at[pl.ds(k * width, width), :], wbuf.at[k % 2, :, pl.ds(j * each, each)], wsem.at[k % 2, j])
            for j, w in enumerate(weights)
        ]

    for k in range(2):
        for c in weight_copies(k):
            c.start()

    met = _greet((partner, right, left))

    def squares(k, total):
        wide = x_ref[:, pl.ds(k * width, width)].astype(F32)
        return total + jnp.sum(wide * wide, -1, keepdims=True)

    total = lax.fori_loop(0, pieces, squares, jnp.zeros((own, 1), F32))
    scale = lax.rsqrt(total * (1 / (pieces * width)) + 1e-6)
    mine = pl.multiple_of(me * own, own)

    def norm(k, _):
        here = pl.ds(k * width, width)
        xg[k, pl.ds(mine, own), :] = (x_ref[:, here].astype(F32) * scale * gain_ref[here].astype(F32)[None, :]).astype(BF16)

    lax.fori_loop(0, 2, norm, None)
    def copy(k, m, owner, low, size, to):
        block = xg.at[k, pl.ds(pl.multiple_of(owner * own + low, half), size), :]
        return pltpu.make_async_remote_copy(block, block, ssem.at[k, m], rsem.at[k, m], device_id={"tp": to}, device_id_type=MESH)

    across = lambda other: other + 1 - 2 * core
    opp2, left2, right2 = across(opposite), across(left), across(right)

    sent = (
        (me, 0, own, partner),
        (me, 0, own, right),
        (me, 0, own, left),
        (left, 0, half, right),
        (right, half, half, left),
        (left, 0, own, partner),
        (right, 0, own, partner),
        (opposite, 0, half, partner),
        (opposite, half, half, partner),
    )
    landed = (
        (partner, 0, own, partner),
        (left, 0, own, partner),
        (right, 0, own, partner),
        (opposite, 0, half, partner),
        (opposite, half, half, partner),
        (left2, 0, own, partner),
        (right2, 0, own, partner),
        (opp2, 0, half, partner),
        (opp2, half, half, partner),
    )

    def start(k, *which):
        for m in which:
            copy(k, m, *sent[m]).start()

    def await_(k, *which):
        for m in which:
            copy(k, m, *landed[m]).wait_recv()

    met()
    for k in range(2):
        start(k, 1, 2, 0)
    lax.fori_loop(2, pieces, norm, None)
    acc[...] = jnp.zeros_like(acc)

    def step(s, _):
        @pl.when((s >= lag[0]) & (s < pieces + lag[0]))
        def _():
            k = s - lag[0]
            await_(k, 1)
            start(k, 3, 5)
            await_(k, 2)
            start(k, 4, 6)

        @pl.when((s >= lag[1]) & (s < pieces + lag[1]))
        def _():
            k = s - lag[1]
            await_(k, 3)
            start(k, 7)
            await_(k, 4)
            start(k, 8)

        @pl.when((s >= 2) & (s < pieces))
        def _():
            start(s, 1, 2, 0)

        @pl.when(s >= lag[2])
        def _():
            k = s - lag[2]
            await_(k, 0, 5, 6, 7, 8)
            for c in weight_copies(k):
                c.wait()

            def columns(t, _):
                here = pl.ds(pl.multiple_of(t * tile, tile), tile)
                acc[:, here] += _dot(xg[k], wbuf[k % 2, :, here], 1, 0)

            lax.fori_loop(0, acc.shape[1] // tile, columns, None)

            @pl.when(k + 2 < pieces)
            def _():
                for c in weight_copies(k + 2):
                    c.start()

    lax.fori_loop(0, pieces + lag[2], step, None)
    finish(acc, wbuf, extra, outs, osem)

    def drain(k, _):
        for m in range(len(sent)):
            copy(k, m, *sent[m]).wait_send()

    lax.fori_loop(0, pieces, drain, None)


class _Blocks:
    def __init__(self, parts, outs, extra):
        self.parts, self.outs, self.extra = parts, outs, extra

    def __call__(self, acc, wbuf, extra, outs, osem):
        rows = wbuf.shape[1] // 2
        each = outs[0].shape[1]
        copies = []
        for b in range(acc.shape[0] // rows):
            low, first = (b % 2) * rows, 0
            for groups, values in self.parts:

                def columns(t, _):
                    at = pl.multiple_of(t * WIDE, WIDE)
                    wbuf[b // 2, low : low + rows, pl.ds(at, WIDE)] = values(acc, extra, b * rows, rows, at)

                lax.fori_loop(first, first + groups, columns, None)
                first += groups
            for j, out in enumerate(outs):
                c = pltpu.make_async_copy(
                    wbuf.at[b // 2, pl.ds(low, rows), pl.ds(j * each, each)], out.at[pl.ds(b * rows, rows), :], osem.at[b, j]
                )
                c.start()
                copies.append(c)
        for c in copies:
            c.wait()


def _gather(n, collective_id, x, gain, weights, finish, tile, lag, extra, out_columns):
    own, depth = x.shape
    rows, each, count = own * n, weights[0].shape[1], len(weights)
    pieces = depth // PIECE
    vmem, hbm = pl.BlockSpec(memory_space=pltpu.VMEM), pl.BlockSpec(memory_space=pl.ANY)
    return pl.pallas_call(
        functools.partial(_gather_kernel, n, count, finish, tile, lag),
        out_shape=[jax.ShapeDtypeStruct((rows, out_columns), BF16)] * finish.outs,
        in_specs=[vmem, vmem] + [hbm] * count + [vmem] * finish.extra,
        out_specs=[hbm] * finish.outs,
        scratch_shapes=[
            pltpu.VMEM((pieces, rows, PIECE), BF16),
            pltpu.VMEM((rows, each * count), F32),
            pltpu.VMEM((2, PIECE, each * count), BF16),
            pltpu.SemaphoreType.DMA((2, count)),
            pltpu.SemaphoreType.DMA((4, finish.outs)),
            pltpu.SemaphoreType.DMA((pieces, 9)),
            pltpu.SemaphoreType.DMA((pieces, 9)),
        ],
        compiler_params=pltpu.CompilerParams(collective_id=collective_id, has_side_effects=True, vmem_limit_bytes=VMEM),
        cost_estimate=pl.CostEstimate(
            flops=2 * rows * depth * each * count, bytes_accessed=2 * depth * each * count, transcendentals=rows * each
        ),
    )(x, gain, *weights, *extra)


def _scatter_kernel(n, lag, a_ref, w_ref, x_ref, o_ref, a_v, wbuf, keep, d_out, d_in, a_out, a_in, b_out, b_in, asem, wsem, ssem, rsem):
    pieces, width = d_in.shape[0], wbuf.shape[2]
    slots, own = keep.shape[0], keep.shape[2]
    half = own // 2
    chips = n // 2
    me, core, partner, right, left, opposite = _place(n)

    def weight_copy(k):
        here = pl.ds(pl.multiple_of(k * width, width), width)
        return pltpu.make_async_copy(w_ref.at[:, here], wbuf.at[k % 3], wsem.at[k % 3])

    fetch = pltpu.make_async_copy(a_ref, a_v, asem)
    fetch.start()
    for k in range(2):
        weight_copy(k).start()
    met = _greet((partner, right, left))

    def copy(k, m, source, target, to):
        return pltpu.make_async_remote_copy(source, target, ssem.at[k, m], rsem.at[k, m], device_id={"tp": to}, device_id_type=MESH)

    def cores(k):
        return copy(k, 0, d_out.at[k % 2], d_in.at[k], partner)

    def far(k):
        return [
            copy(k, 1, a_out.at[k % 2, pl.ds(0, half)], a_in.at[k, pl.ds(0, half)], right),
            copy(k, 2, a_out.at[k % 2, pl.ds(half, half)], a_in.at[k, pl.ds(half, half)], left),
        ]

    def near(k):
        return [copy(k, 3, b_out.at[k % 2, 0], b_in.at[k, 0], right), copy(k, 4, b_out.at[k % 2, 1], b_in.at[k, 1], left)]

    def term(k, owner, low=0, size=own):
        here = pl.ds(low, size)
        return keep[k % slots, owner, here, :] + d_in[k, owner // 2, here, :].astype(F32)

    fetch.wait()
    met()

    def step(s, _):
        @pl.when(s < pieces)
        def _():
            weight_copy(s).wait()

            @pl.when(s + 2 < pieces)
            def _():
                weight_copy(s + 2).start()

            keep[s % slots] = _dot(a_v[...], wbuf[s % 3], 1, 0).reshape(n, own, width)

            @pl.when(s >= 2)
            def _():
                cores(s - 2).wait_send()

            for q in range(chips):
                d_out[s % 2, q] = keep[s % slots, 2 * q + 1 - core].astype(BF16)

        @pl.when((s >= lag[0]) & (s < pieces + lag[0]))
        def _():
            k = s - lag[0]
            cores(k).wait_recv()

            @pl.when(k >= 2)
            def _():
                for c in far(k - 2):
                    c.wait_send()

            a_out[k % 2] = term(k, opposite).astype(BF16)

        @pl.when(s < pieces)
        def _():
            cores(s).start()

        @pl.when((s >= lag[1]) & (s < pieces + lag[1]))
        def _():
            k = s - lag[1]
            for c in far(k):
                c.wait_recv()

            @pl.when(k >= 2)
            def _():
                for c in near(k - 2):
                    c.wait_send()

            b_out[k % 2, 0, pl.ds(0, half)] = (term(k, right, 0, half) + a_in[k, pl.ds(0, half)].astype(F32)).astype(BF16)
            b_out[k % 2, 0, pl.ds(half, half)] = term(k, right, half, half).astype(BF16)
            b_out[k % 2, 1, pl.ds(0, half)] = term(k, left, 0, half).astype(BF16)
            b_out[k % 2, 1, pl.ds(half, half)] = (term(k, left, half, half) + a_in[k, pl.ds(half, half)].astype(F32)).astype(BF16)

        @pl.when((s >= lag[0]) & (s < pieces + lag[0]))
        def _():
            for c in far(s - lag[0]):
                c.start()

        @pl.when(s >= lag[2])
        def _():
            k = s - lag[2]
            for c in near(k):
                c.wait_recv()
            here = pl.ds(pl.multiple_of(k * width, width), width)
            total = term(k, me) + b_in[k, 0].astype(F32) + b_in[k, 1].astype(F32)
            o_ref[:, here] = (x_ref[:, here].astype(F32) + total).astype(BF16)

        @pl.when((s >= lag[1]) & (s < pieces + lag[1]))
        def _():
            for c in near(s - lag[1]):
                c.start()

    lax.fori_loop(0, pieces + lag[2], step, None)
    for k in (pieces - 2, pieces - 1):
        for c in [cores(k), *far(k), *near(k)]:
            c.wait_send()


def _scatter(n, collective_id, a, w, x):
    rows, depth = a.shape
    own, columns = x.shape
    pieces = columns // PIECE
    vmem, hbm = pl.BlockSpec(memory_space=pltpu.VMEM), pl.BlockSpec(memory_space=pl.ANY)
    return pl.pallas_call(
        functools.partial(_scatter_kernel, n, SCATTER_LAG),
        out_shape=jax.ShapeDtypeStruct((own, columns), BF16),
        in_specs=[hbm, hbm, vmem],
        out_specs=vmem,
        scratch_shapes=[
            pltpu.VMEM((rows, depth), BF16),
            pltpu.VMEM((3, depth, PIECE), BF16),
            pltpu.VMEM((SCATTER_LAG[2] + 1, n, own, PIECE), F32),
            pltpu.VMEM((2, n // 2, own, PIECE), BF16),
            pltpu.VMEM((pieces, n // 2, own, PIECE), BF16),
            pltpu.VMEM((2, own, PIECE), BF16),
            pltpu.VMEM((pieces, own, PIECE), BF16),
            pltpu.VMEM((2, 2, own, PIECE), BF16),
            pltpu.VMEM((pieces, 2, own, PIECE), BF16),
            pltpu.SemaphoreType.DMA,
            pltpu.SemaphoreType.DMA((3,)),
            pltpu.SemaphoreType.DMA((pieces, 5)),
            pltpu.SemaphoreType.DMA((pieces, 5)),
        ],
        compiler_params=pltpu.CompilerParams(collective_id=collective_id, has_side_effects=True, vmem_limit_bytes=VMEM),
        cost_estimate=pl.CostEstimate(flops=2 * rows * depth * columns, bytes_accessed=2 * depth * columns, transcendentals=0),
    )(a, w, x)


def _attend_kernel(n, bk, scale, q_ref, k_ref, v_ref, w_ref, x_ref, o_ref, q_v, k_v, v_v, w_v, seen, top_s, mix_s, keep, d_out, d_in,
                   a_out, a_in, b_in, lsem, wsem, dsend, drecv, ssem, rsem):
    heads = top_s.shape[0]
    pieces, own, width = a_in.shape
    half, both = own // 2, 2 * own
    me, core, partner, right, left, opposite = _place(n)
    order = (opposite // 2, right // 2, left // 2, me // 2)

    fetches = [pltpu.make_async_copy(r, t, lsem.at[i]) for i, (r, t) in enumerate(((k_ref, k_v), (v_ref, v_v)))]
    queries = [
        pltpu.make_async_copy(q_ref.at[pl.ds(pl.multiple_of(c * both, both), both), :], q_v.at[i], lsem.at[2 + i])
        for i, c in enumerate(order)
    ]
    for c in queries[:1] + fetches:
        c.start()

    def weight_copy(j):
        return pltpu.make_async_copy(w_ref.at[:, pl.ds(pl.multiple_of(j * width, width), width)], w_v.at[j], wsem.at[j])

    def loop(f):
        lax.fori_loop(0, pieces, lambda j, _: f(j), None)

    loop(lambda j: weight_copy(j).start())
    for c in queries[1:]:
        c.start()
    met = _greet((partner, right, left))
    for c in fetches:
        c.wait()

    e = scale * LOG2E
    ones = jnp.ones((8, bk), BF16)
    gap = lax.broadcasted_iota(jnp.int32, (bk, both), 1) - lax.broadcasted_iota(jnp.int32, (bk, both), 0)
    part = lambda i: slice(i * HEAD, (i + 1) * HEAD)

    def attend(stage):
        chip = order[stage]
        queries[stage].wait()
        top_s[...] = jnp.full(top_s.shape, NEG, F32)
        mix_s[...] = jnp.zeros(mix_s.shape, F32)

        def block(j, masked):
            here = pl.ds(pl.multiple_of(j * bk, bk), bk)
            scores = [_dot(k_v[here, part(i)], q_v[stage, :, part(i)], 1, 1) for i in range(heads)]
            weights, keeps = [], []
            for i, s in enumerate(scores):
                if masked:
                    s = jnp.where(gap >= j * bk - chip * both, s, HIDDEN)
                old = top_s[i : i + 1, :]
                top = jnp.maximum(old, s.max(axis=0, keepdims=True))
                top_s[i : i + 1, :] = top
                weights.append(jnp.exp2((s - top) * e).astype(BF16))
                keeps.append(jnp.exp2((old - top) * e))
            for i, (p, keep_) in enumerate(zip(weights, keeps)):
                values = jnp.concatenate([v_v[here, part(i)].T, ones], axis=0)
                mix_s[i] = mix_s[i] * keep_ + _dot(values, p, 1, 0)

        whole = chip * (both // bk)
        lax.fori_loop(0, whole, lambda j, _: block(j, False), None)
        lax.fori_loop(whole, whole + both // bk, lambda j, _: block(j, True), None)
        for i in range(heads):
            total = mix_s[i, HEAD : HEAD + 1, :]
            seen[:, part(i)] = (mix_s[i, :HEAD, :] * (1 / total)).T.astype(BF16)

    def d_target(stage, j):
        return a_out.at[j] if stage == 3 else d_out.at[stage % 2, j]

    def cores(stage, j):
        return pltpu.make_async_remote_copy(
            d_target(stage, j), d_in.at[stage, j], dsend.at[stage, j], drecv.at[stage, j], device_id={"tp": partner}, device_id_type=MESH
        )

    def copy(j, m, source, target, to):
        return pltpu.make_async_remote_copy(source, target, ssem.at[j, m], rsem.at[j, m], device_id={"tp": to}, device_id_type=MESH)

    low, high = pl.ds(0, half), pl.ds(half, half)

    def far(j):
        return [copy(j, 0, a_out.at[j, low], a_in.at[j, low], right), copy(j, 1, a_out.at[j, high], a_in.at[j, high], left)]

    def near(j, side):
        return copy(j, 2 + side, d_out.at[side, j], b_in.at[j, side], (right, left)[side])

    def term(stage, j, rows):
        return keep[stage % 3, j, rows, :] + d_in[stage, j, rows, :].astype(F32)

    def multiply(stage, j):
        both_rows = _dot(seen[...], w_v[j], 1, 0).reshape(2, own, width)
        mix = jnp.where(core == 0, both_rows[0], both_rows[1])
        keep[stage % 3, j] = mix
        d_target(stage, j)[...] = jnp.where(core == 0, both_rows[1], both_rows[0]).astype(BF16)

    every = pl.ds(0, own)

    def first(j):
        cores(0, j).wait_recv()
        a_out[j] = term(0, j, every).astype(BF16)

    attend(0)
    met()

    def opening(j, _):
        @pl.when(j < pieces)
        def _():
            weight_copy(j).wait()
            multiply(0, j)

        @pl.when((j >= 2) & (j < pieces + 2))
        def _():
            first(j - 2)

        @pl.when(j < pieces)
        def _():
            cores(0, j).start()

        @pl.when(j >= 3)
        def _():
            for c in far(j - 3):
                c.start()

    lax.fori_loop(0, pieces + 3, opening, None)

    def terms(stage):
        attend(stage)

        def term_piece(j, _):
            @pl.when(j < pieces)
            def _():
                if stage == 2:
                    cores(0, j).wait_send()
                if stage == 3:
                    for c in far(j):
                        c.wait_send()
                multiply(stage, j)

            @pl.when(j >= 1)
            def _():
                cores(stage, j - 1).start()

        lax.fori_loop(0, pieces + 1, term_piece, None)

    def second(j, _):
        @pl.when(j < pieces)
        def _():
            for c in far(j):
                c.wait_recv()
            cores(1, j).wait_recv()
            cores(2, j).wait_recv()
            cores(1, j).wait_send()
            cores(2, j).wait_send()
            d_out[0, j, low] = (term(1, j, low) + a_in[j, low].astype(F32)).astype(BF16)
            d_out[0, j, high] = term(1, j, high).astype(BF16)
            d_out[1, j, low] = term(2, j, low).astype(BF16)
            d_out[1, j, high] = (term(2, j, high) + a_in[j, high].astype(F32)).astype(BF16)

        @pl.when(j >= 1)
        def _():
            near(j - 1, 0).start()
            near(j - 1, 1).start()

    terms(1)
    terms(2)
    lax.fori_loop(0, pieces + 1, second, None)
    terms(3)

    def third(j):
        cores(3, j).wait_recv()
        near(j, 0).wait_recv()
        near(j, 1).wait_recv()
        here = pl.ds(pl.multiple_of(j * width, width), width)
        total = term(3, j, every) + b_in[j, 0].astype(F32) + b_in[j, 1].astype(F32)
        o_ref[:, here] = (x_ref[:, here].astype(F32) + total).astype(BF16)

    loop(third)

    def drain(j):
        for c in (cores(3, j), near(j, 0), near(j, 1)):
            c.wait_send()

    loop(drain)


def _attend(n, collective_id, q, k, v, w, x, bk=256, width=1024):
    rows, depth = q.shape
    own, columns = x.shape
    pieces, heads, both = columns // width, depth // HEAD, 2 * own
    vmem, hbm = pl.BlockSpec(memory_space=pltpu.VMEM), pl.BlockSpec(memory_space=pl.ANY)
    return pl.pallas_call(
        functools.partial(_attend_kernel, n, bk, HEAD**-0.5),
        out_shape=jax.ShapeDtypeStruct((own, columns), BF16),
        in_specs=[hbm, hbm, hbm, hbm, vmem],
        out_specs=vmem,
        scratch_shapes=[
            pltpu.VMEM((n // 2, both, depth), BF16),
            pltpu.VMEM((rows, depth), BF16),
            pltpu.VMEM((rows, depth), BF16),
            pltpu.VMEM((pieces, depth, width), BF16),
            pltpu.VMEM((both, depth), BF16),
            pltpu.VMEM((heads, both), F32),
            pltpu.VMEM((heads, HEAD + 8, both), F32),
            pltpu.VMEM((3, pieces, own, width), F32),
            pltpu.VMEM((2, pieces, own, width), BF16),
            pltpu.VMEM((n // 2, pieces, own, width), BF16),
            pltpu.VMEM((pieces, own, width), BF16),
            pltpu.VMEM((pieces, own, width), BF16),
            pltpu.VMEM((pieces, 2, own, width), BF16),
            pltpu.SemaphoreType.DMA((2 + n // 2,)),
            pltpu.SemaphoreType.DMA((pieces,)),
            pltpu.SemaphoreType.DMA((n // 2, pieces)),
            pltpu.SemaphoreType.DMA((n // 2, pieces)),
            pltpu.SemaphoreType.DMA((pieces, 4)),
            pltpu.SemaphoreType.DMA((pieces, 4)),
        ],
        compiler_params=pltpu.CompilerParams(collective_id=collective_id, has_side_effects=True, vmem_limit_bytes=VMEM),
        cost_estimate=pl.CostEstimate(
            flops=4 * rows * rows * depth + 2 * rows * depth * columns, bytes_accessed=2 * depth * columns, transcendentals=heads * rows * rows
        ),
    )(q, k, v, w, x)


def _tables(rows):
    half = HEAD // 2
    rate = (np.float32(THETA) ** (-np.arange(half, dtype=np.float32) / np.float32(half))).astype(np.float32)
    angle = np.arange(rows, dtype=np.float32)[:, None] * rate
    cos, sin = np.cos(angle.astype(np.float64)), np.sin(angle.astype(np.float64))
    return np.concatenate([cos, cos], 1).astype(np.float32), np.concatenate([-sin, sin], 1).astype(np.float32)


def _turned(acc, extra, low, rows, at):
    cos, sin = (r[low : low + rows, :] for r in extra)
    heads = []
    for i in range(0, WIDE, HEAD):
        wide = acc[low : low + rows, pl.ds(at + i, HEAD)].astype(BF16).astype(F32)
        heads.append((wide * cos + pltpu.roll(wide, HEAD // 2, 1) * sin).astype(BF16))
    return jnp.concatenate(heads, 1)


def _plain(acc, extra, low, rows, at):
    return acc[low : low + rows, pl.ds(at, WIDE)].astype(BF16)


def _hidden(acc, extra, low, rows, at):
    gate = acc[low : low + rows, pl.ds(at, WIDE)]
    up = acc[low : low + rows, pl.ds(at + acc.shape[1] // 2, WIDE)]
    return (gate * lax.logistic(gate) * up).astype(BF16)


def solution(mesh):
    n = mesh.shape["tp"]

    def step(x, gain_a, wq, wk, wv, wo, gain_m, w_gate, w_up, w_down):
        rows = x.shape[0] * n
        tables = [jnp.asarray(t) for t in _tables(rows)]
        q, k, v = _gather(n, 0, x, gain_a, (wq, wk, wv), _Blocks([(2 * wq.shape[1] // WIDE, _turned), (wv.shape[1] // WIDE, _plain)], 3, 2), 3072, GATHER_LAG, tables, wq.shape[1])
        h = _attend(n, 1, q, k, v, wo, x)
        (hidden,) = _gather(n, 2, h, gain_m, (w_gate, w_up), _Blocks([(w_gate.shape[1] // WIDE, _hidden)], 1, 0), 2048, SHORT_LAG, (), w_gate.shape[1])
        return _scatter(n, 3, hidden, w_down, h)

    tokens, columns, rows_of = P(("dp", "tp"), None), P(None, "tp"), P("tp", None)
    return jax.shard_map(
        step,
        mesh=mesh,
        in_specs=(tokens, P(None), columns, columns, columns, rows_of, P(None), columns, columns, rows_of),
        out_specs=tokens,
        check_vma=False,
    )
```
